768 devices in a mesh: replica: 8 (over x, core), fsdp: 24 (over y_lo, z), tensor: 4 (over y_hi).
Axes of the slice: x: 4, y: 8 (y_hi: 4, y_lo: 2; y = y_hi * 2 + y_lo), z: 12, core: 2. Of those that a mesh axis runs over, the one named last changes fastest.
Arguments:
- pseudo_grad: bfloat16 [8, 3072, 18432], P('replica', 'fsdp', 'tensor'), may hold values from -6 to 6
- compensation: float32 [8, 3072, 18432], P('replica', 'fsdp', 'tensor'), may hold values from -6 to 6
- params: float32 [3072, 18432], P(('fsdp', 'replica'), 'tensor'), may hold values from -6 to 6
- momentum: float32 [3072, 18432], P(('fsdp', 'replica'), 'tensor'), may hold values from -6 to 6
- probe: bfloat16 [1536, 18432], P('fsdp', 'tensor'), may hold values from -0.046875 to 0.046875
Outputs:
- new_params: float32 [3072, 18432], P(('fsdp', 'replica'), 'tensor')
- new_momentum: float32 [3072, 18432], P(('fsdp', 'replica'), 'tensor')
- probe_out: bfloat16 [1536, 3072], P('tensor', 'fsdp')
The draws below stay inside these ranges and needn't reach their ends.
All inputs are finite; a program needn't handle non-finite values.
Results may differ from the reference program's by a relative error of at most 0.014.
Values may be sent and summed in bfloat16 or wider, within the bound.
No kernel may reach another device: no remote copies, remote signals or barrier semaphores. Data moves between devices by JAX's collectives and lax.ppermute only.
A program may use at most 64 MiB of HBM per device.

```python
import jax
import jax.numpy as jnp
from jax import lax

D = 3072
FW = 18432
PROBE = 1536
N_REPLICA = 8


def steps_of(key, shape, split, smallest, high):
    def one(axis_at, parts):
        draws = jax.random.uniform(jax.random.fold_in(jax.random.fold_in(key, 6), axis_at), (parts,), jnp.float32, smallest / len(split), high / len(split))
        return jnp.repeat(jnp.exp(draws), shape[axis_at] // parts).reshape((-1,) + (1,) * (len(shape) - axis_at - 1))

    loudness = one(*split[0])
    for cut in split[1:]:
        loudness = loudness * one(*cut)
    return loudness


def centred(rng, dims, deviation, limit, shards=(), held_as=jnp.bfloat16):
    entries = jax.random.normal(rng, dims, jnp.float32) * deviation
    if len(shards) > 0:
        entries = steps_of(rng, dims, shards, -0.22, 0.18) * entries
    return jnp.clip(entries, min=-limit, max=limit).astype(held_as)


def setup_inputs(seed: int = 0) -> dict:
    key_list = jax.random.split(jax.random.key(seed), 6)
    pseudo_grad = centred(key_list[0], (N_REPLICA, D, FW), 1.0, 6.0, ((0, 8), (1, 24), (2, 4)))
    compensation = centred(key_list[1], (N_REPLICA, D, FW), 1.0, 6.0, ((0, 8), (1, 24), (2, 4)), jnp.float32)
    params = centred(key_list[2], (D, FW), 1.0, 6.0, ((0, 192), (1, 4)), jnp.float32)
    momentum = centred(key_list[3], (D, FW), 1.0, 6.0, ((0, 192), (1, 4)), jnp.float32)
    probe = centred(key_list[4], (PROBE, FW), FW ** -0.5, 0.046875, ((0, 24), (1, 4)))
    return dict(pseudo_grad=pseudo_grad, compensation=compensation, params=params, momentum=momentum, probe=probe)


outer_rate = 0.7
nesterov = 0.9


def reference(pseudo_grad, compensation, params, momentum, probe):
    def accumulate(summed, pair):
        grads, carried = pair
        outgoing = (grads.astype(jnp.float32) + carried).astype(jnp.bfloat16)
        outgoing = lax.optimization_barrier(outgoing)
        return summed + outgoing.astype(jnp.float32), None

    start = jnp.zeros(params.shape, jnp.float32)
    summed, _ = lax.scan(accumulate, start, (pseudo_grad, compensation))
    average = summed / N_REPLICA
    new_momentum = nesterov * momentum + average
    new_params = params - outer_rate * (average + nesterov * new_momentum)
    weights = new_params.astype(jnp.bfloat16)
    probe_out = lax.dot_general(probe, weights, (((1,), (1,)), ((), ())), preferred_element_type=jnp.float32)
    return new_params, new_momentum, probe_out.astype(jnp.bfloat16)
```

```python
import functools

import jax
import jax.numpy as jnp
from jax import lax
from jax.experimental import pallas as pl
from jax.experimental.pallas import tpu as pltpu
from jax.sharding import Mesh
from jax.sharding import PartitionSpec as P


outer_rate = 0.7
nesterov = 0.9
f32, bf16 = jnp.float32, jnp.bfloat16

X, CORE, YLO, ZQ, ZR, YHI = 4, 2, 2, 4, 3, 4
Z = ZQ * ZR
Z_ORDER = [0, 1, 2, 3, 4, 5, 6, 7]
Y_ORDER = [4, 3, 2, 1, 0, 7, 6, 5]
X_ORDER = [2, 3, 0, 1]
ROWS = 16
COLS = 1152


def exchange(tiles, axes, order):
    return lax.all_to_all(tiles, axes, split_axis=0, concat_axis=0, tiled=True, axis_index_groups=[order])


def shifted(x, axes, n, by):
    return lax.ppermute(x, axes, [(i, (i + by) % n) for i in range(n)])


def taken(tiles, i):
    return lax.dynamic_index_in_dim(tiles, i, 0, keepdims=False)


VMEM = pl.BlockSpec(memory_space=pltpu.VMEM)
ANY = pl.BlockSpec(memory_space=pltpu.HBM)
SMALL = pltpu.CompilerParams(vmem_limit_bytes=8 << 20)


def spread(probe_ref, copies_ref, kept_ref, sems):
    core, at = lax.axis_index("core"), pl.multiple_of(lax.axis_index("x") * COLS, 128)
    loads, stores = [], []
    for ylo in range(YLO):
        row = pl.multiple_of((core * YLO + ylo) * 16, 16)
        source = probe_ref.at[pl.ds(row, 16), pl.ds(at, COLS)]
        loads.append(pltpu.make_async_copy(source, kept_ref.at[ylo], sems.at[ylo]))
        loads[-1].start()
    for ylo in range(YLO):
        loads[ylo].wait()
        for zq in range(ZQ):
            n = Z_ORDER.index(ylo * ZQ + zq)
            stores.append(pltpu.make_async_copy(kept_ref.at[ylo], copies_ref.at[n], sems.at[YLO + n]))
            stores[-1].start()
    for store in stores:
        store.wait()


def added(other, grads_ref, carried_ref, sums_ref, grad_ref, carry_ref, sems):
    core = lax.axis_index("core")
    half = 1 - core if other else core
    copies = []
    for x in range(X):
        row = pl.multiple_of((x * CORE + half) * ROWS, 16)
        pair = (
            pltpu.make_async_copy(grads_ref.at[0, pl.ds(row, ROWS)], grad_ref.at[x], sems.at[0, x]),
            pltpu.make_async_copy(carried_ref.at[0, pl.ds(row, ROWS)], carry_ref.at[x], sems.at[1, x]),
        )
        for copy in pair:
            copy.start()
        copies.append(pair)
    for x in range(X):
        for copy in copies[x]:
            copy.wait()
        sums_ref[x * ROWS : (x + 1) * ROWS] = (grad_ref[x].astype(f32) + carry_ref[x]).astype(bf16)


def outgoing(other, grads, carried):
    return pl.pallas_call(
        functools.partial(added, other),
        out_shape=jax.ShapeDtypeStruct((X * ROWS, X * COLS), bf16),
        in_specs=[ANY, ANY],
        out_specs=VMEM,
        scratch_shapes=[
            pltpu.VMEM((X, ROWS, X * COLS), bf16),
            pltpu.VMEM((X, ROWS, X * COLS), f32),
            pltpu.SemaphoreType.DMA((2, X)),
        ],
        name="lent" if other else "kept",
        compiler_params=SMALL,
    )(pltpu.with_memory_space_constraint(grads, pltpu.HBM), pltpu.with_memory_space_constraint(carried, pltpu.HBM))


def product(below_ref, far_ref, above_ref, gathered_ref, chunks_ref, weights_ref):
    for ylo in range(YLO):
        for x in range(X):
            for core in range(CORE):
                at = (x * CORE + core) * ROWS
                weights_ref[ylo, at : at + ROWS] = gathered_ref[core * YLO + ylo, x * ROWS : (x + 1) * ROWS]
    for place, ref in enumerate((below_ref, far_ref, above_ref)):
        rows = ref[...].reshape(YLO * ZQ * 16, COLS)
        for ylo in range(YLO):
            found = lax.dot_general(
                rows, weights_ref[ylo], (((1,), (1,)), ((), ())), preferred_element_type=f32
            ).astype(bf16)
            for block in range(YLO * ZQ):
                t, low = block // 2, block % 2
                at = (low * ZR + place) * 16
                row = Z_ORDER.index(block) * 16
                chunks_ref[Y_ORDER.index(t * YLO + ylo), at : at + 16] = found[row : row + 16]


def part_sums(parts_ref, average_ref, sent_ref):
    for ylo in range(YLO):
        total = sum(parts_ref[Y_ORDER.index(t * YLO + ylo)].astype(f32) for t in range(YHI)).astype(bf16)
        for x in range(X):
            sent_ref[x, ylo * 96 : (ylo + 1) * 96] = total
    for x in range(X):
        for k in range(9):
            at = YLO * 96 + k * ROWS
            sent_ref[X_ORDER.index(x), at : at + ROWS] = average_ref[x * ROWS : (x + 1) * ROWS, k * 128 : (k + 1) * 128]


def updates(joined_ref, params_ref, momentum_ref, half_ref, new_params_ref, new_momentum_ref):
    total = joined_ref[0, 0 : YLO * 96].astype(f32)
    for x in range(1, X):
        total = total + joined_ref[x, 0 : YLO * 96].astype(f32)
    half_ref[...] = total.astype(bf16)
    for x in range(X):
        for k in range(9):
            at, col = YLO * 96 + k * ROWS, x * COLS + k * 128
            average = joined_ref[X_ORDER.index(x), at : at + ROWS].astype(f32)
            moved = nesterov * momentum_ref[:, col : col + 128] + average
            new_momentum_ref[:, col : col + 128] = moved
            new_params_ref[:, col : col + 128] = params_ref[:, col : col + 128] - outer_rate * (
                average + nesterov * moved
            )


def placing(whole_ref, out_ref):
    for place in range(ZR):
        zr = lax.rem(lax.axis_index("zr") + (place + ZR - 1), ZR)
        for core in range(CORE):
            for ylo in range(YLO):
                for low in range(2):
                    row = (low * ZR + zr) * 64 + (core * YLO + ylo) * 16
                    at = ylo * 96 + (low * ZR + place) * 16
                    out_ref[pl.ds(pl.multiple_of(row, 16), 16)] = whole_ref[core, at : at + 16]


def per_device(pseudo_grad, compensation, params, momentum, probe):
    x = lax.axis_index("x")

    copies = pl.pallas_call(
        spread,
        out_shape=jax.ShapeDtypeStruct((YLO * ZQ, 16, COLS), bf16),
        in_specs=[ANY],
        out_specs=ANY,
        scratch_shapes=[pltpu.VMEM((YLO, 16, COLS), bf16), pltpu.SemaphoreType.DMA((YLO + YLO * ZQ,))],
        name="spread",
        compiler_params=SMALL,
    )(pltpu.with_memory_space_constraint(probe, pltpu.HBM))
    far = exchange(copies, ("ylo", "zq"), Z_ORDER)
    below = shifted(far, ("zq", "zr"), Z, 1)
    above = shifted(far, ("zq", "zr"), Z, -1)

    partners = shifted(outgoing(True, pseudo_grad, compensation), "core", CORE, 1)
    kept = outgoing(False, pseudo_grad, compensation)
    pair = (partners.astype(f32) + kept).astype(bf16)
    decayed = (params - (outer_rate * nesterov * nesterov) * momentum).astype(bf16)
    both = jnp.concatenate([pair, decayed], axis=0)

    def share(i):
        return lax.dynamic_slice_in_dim(both, lax.rem(x + i, X) * COLS, COLS, axis=1)

    arrived = [share(0)]
    for i in range(1, X):
        arrived.append(shifted(share(i), "x", X, i))
    average = sum(a[: X * ROWS].astype(f32) for a in arrived) / (X * CORE)
    places = jnp.stack([a[X * ROWS :] for a in arrived])
    base = jnp.concatenate([taken(places, lax.rem(x - i + X, X)) for i in range(X)]).astype(f32)
    weights = (base - (outer_rate * (1 + nesterov)) * average).astype(bf16)

    two = lax.all_gather(weights, "ylo", axis=0)
    local_weights = lax.all_gather(two, "core", axis=0)
    chunks = pl.pallas_call(
        product,
        out_shape=jax.ShapeDtypeStruct((YHI * YLO, 96, 128), bf16),
        in_specs=[VMEM] * 4,
        out_specs=VMEM,
        scratch_shapes=[pltpu.VMEM((YLO, 128, COLS), bf16)],
        name="product",
        compiler_params=SMALL,
    )(below, far, above, local_weights.reshape(CORE * YLO, X * ROWS, COLS))
    parts = exchange(chunks, ("yhi", "ylo"), Y_ORDER)
    sent = pl.pallas_call(
        part_sums,
        out_shape=jax.ShapeDtypeStruct((X, YLO * 96 + 9 * ROWS, 128), bf16),
        in_specs=[VMEM] * 2,
        out_specs=VMEM,
        name="part_sums",
        compiler_params=SMALL,
    )(parts, average.astype(bf16))
    joined = exchange(sent, "x", X_ORDER)
    half, new_params, new_momentum = pl.pallas_call(
        updates,
        out_shape=(
            jax.ShapeDtypeStruct((YLO * 96, 128), bf16),
            jax.ShapeDtypeStruct(params.shape, f32),
            jax.ShapeDtypeStruct(momentum.shape, f32),
        ),
        in_specs=[VMEM] * 3,
        out_specs=(VMEM,) * 3,
        name="updates",
        compiler_params=SMALL,
    )(joined, params, momentum)
    whole = lax.all_gather(half, "core", axis=0)
    probe_out = pl.pallas_call(
        placing,
        out_shape=jax.ShapeDtypeStruct((384, 128), bf16),
        in_specs=[VMEM],
        out_specs=VMEM,
        name="placing",
        compiler_params=SMALL,
    )(whole)
    return new_params, new_momentum, probe_out


def solution(mesh):
    fine = Mesh(
        mesh.devices.reshape(X, CORE, YLO, ZQ, ZR, YHI), ("x", "core", "ylo", "zq", "zr", "yhi")
    )
    whole, rows = ("x", "core"), ("ylo", "zq", "zr")
    shard = P((*rows, *whole), "yhi")
    in_specs = (P(whole, rows, "yhi"), P(whole, rows, "yhi"), shard, shard, P(rows, "yhi"))
    out_specs = (shard, shard, P("yhi", rows))

    return jax.shard_map(per_device, mesh=fine, in_specs=in_specs, out_specs=out_specs, check_vma=False)
```

```python
import jax
import jax.numpy as jnp
from jax import lax
from jax.experimental import pallas as pl
from jax.experimental.pallas import tpu as pltpu
from jax.sharding import Mesh
from jax.sharding import PartitionSpec as P


outer_rate = 0.7
nesterov = 0.9
f32, bf16 = jnp.float32, jnp.bfloat16

X, CORE, YLO, ZQ, ZR, YHI = 4, 2, 2, 4, 3, 4
Z = ZQ * ZR
Y_ORDER = [4, 3, 2, 1, 0, 7, 6, 5]
X_ORDER = [2, 0, 1, 3]
ROWS = 16
COLS = 1152


def exchange(tiles, axes, orders):
    return lax.all_to_all(tiles, axes, split_axis=0, concat_axis=0, tiled=True, axis_index_groups=orders)


LEADS = (3, 3, 2)
FAR_ORDERS = [
    [(ylo * ZQ + (lead + n) % ZQ) * ZR + zr for ylo in range(YLO) for n in range(ZQ)] for zr, lead in enumerate(LEADS)
]


def far_place(ylo, zq, zr):
    lead = jnp.where(zr == 0, LEADS[0], jnp.where(zr == 1, LEADS[1], LEADS[2]))
    return ylo * ZQ + lax.rem(zq + ZQ - lead, ZQ)


def swapped(x, axes, pairs):
    return lax.ppermute(x, axes, [*pairs, *((j, i) for i, j in pairs)])


def taken(tiles, i):
    return lax.dynamic_index_in_dim(tiles, i, 0, keepdims=False)


VMEM = pl.BlockSpec(memory_space=pltpu.VMEM)
ANY = pl.BlockSpec(memory_space=pltpu.HBM)
SMALL = pltpu.CompilerParams(vmem_limit_bytes=8 << 20)


def started(other, grads_ref, carried_ref, grad_ref, carry_ref, sems):
    core = lax.axis_index("core")
    half = 1 - core if other else core
    copies = []
    for x in range(X):
        row = pl.multiple_of((x * CORE + half) * ROWS, 16)
        pair = (
            pltpu.make_async_copy(grads_ref.at[0, pl.ds(row, ROWS)], grad_ref.at[x], sems.at[0, x]),
            pltpu.make_async_copy(carried_ref.at[0, pl.ds(row, ROWS)], carry_ref.at[x], sems.at[1, x]),
        )
        for copy in pair:
            copy.start()
        copies.append(pair)
    return copies


def added(copies, sums_ref, grad_ref, carry_ref):
    for x in range(X):
        for copy in copies[x]:
            copy.wait()
        sums_ref[x * ROWS : (x + 1) * ROWS] = (grad_ref[x].astype(f32) + carry_ref[x]).astype(bf16)


def opening(probe_ref, grads_ref, carried_ref, copies_ref, lent_ref, kept_ref, grad_ref, carry_ref, sems, sums_sems):
    core, at = lax.axis_index("core"), pl.multiple_of(lax.axis_index("x") * COLS, 128)
    loads, stores = [], []
    for ylo in range(YLO):
        row = pl.multiple_of((core * YLO + ylo) * 16, 16)
        source = probe_ref.at[pl.ds(row, 16), pl.ds(at, COLS)]
        loads.append(pltpu.make_async_copy(source, kept_ref.at[ylo], sems.at[ylo]))
        loads[-1].start()
    copies = started(True, grads_ref, carried_ref, grad_ref, carry_ref, sums_sems)
    for ylo in range(YLO):
        loads[ylo].wait()
        for zq in range(ZQ):
            to = far_place(ylo, zq, lax.axis_index("zr"))
            stores.append(
                pltpu.make_async_copy(kept_ref.at[ylo], copies_ref.at[to], sems.at[YLO + ylo * ZQ + zq])
            )
            stores[-1].start()
    added(copies, lent_ref, grad_ref, carry_ref)
    for store in stores:
        store.wait()


def own_rows(grads_ref, carried_ref, sums_ref, grad_ref, carry_ref, sems):
    added(started(False, grads_ref, carried_ref, grad_ref, carry_ref, sems), sums_ref, grad_ref, carry_ref)


SUMS = jax.ShapeDtypeStruct((X * ROWS, X * COLS), bf16)
SUMS_SCRATCH = [
    pltpu.VMEM((X, ROWS, X * COLS), bf16),
    pltpu.VMEM((X, ROWS, X * COLS), f32),
]


def neighbour_zr(core):
    zr = lax.axis_index("zr")
    odd = lax.rem(lax.axis_index("zq") * ZR + zr + core, 2)
    return lax.rem(zr + 1 + odd, ZR)


def product(near_ref, far_ref, gathered_ref, chunks_ref, weights_ref, rows_ref):
    for ylo in range(YLO):
        for x in range(X):
            for core in range(CORE):
                at = (x * CORE + core) * ROWS
                weights_ref[ylo, at : at + ROWS] = gathered_ref[core * YLO + ylo, x * ROWS : (x + 1) * ROWS]
    near_zr = neighbour_zr(lax.axis_index("core"))
    for place in range(3):
        for block in range(YLO * ZQ):
            row = (place * YLO * ZQ + block) * 16
            if place < 2:
                rows_ref[row : row + 16] = near_ref[place, far_place(block // ZQ, block % ZQ, near_zr)]
            else:
                rows_ref[row : row + 16] = far_ref[far_place(block // ZQ, block % ZQ, lax.axis_index("zr"))]
    for ylo in range(YLO):
        found = lax.dot_general(
            rows_ref[...], weights_ref[ylo], (((1,), (1,)), ((), ())), preferred_element_type=f32
        ).astype(bf16)
        for place in range(3):
            for block in range(YLO * ZQ):
                t, low = block // 2, block % 2
                at, row = (low * 3 + place) * 16, (place * YLO * ZQ + block) * 16
                chunks_ref[Y_ORDER.index(t * YLO + ylo), at : at + 16] = found[row : row + 16]


def part_sums(parts_ref, average_ref, sent_ref):
    for ylo in range(YLO):
        total = sum(parts_ref[Y_ORDER.index(t * YLO + ylo)].astype(f32) for t in range(YHI)).astype(bf16)
        for x in range(X):
            sent_ref[x, ylo * 96 : (ylo + 1) * 96] = total
    for x in range(X):
        for k in range(9):
            at = YLO * 96 + k * ROWS
            sent_ref[X_ORDER.index(x), at : at + ROWS] = average_ref[x * ROWS : (x + 1) * ROWS, k * 128 : (k + 1) * 128]


def updates(joined_ref, params_ref, momentum_ref, half_ref, new_params_ref, new_momentum_ref):
    total = joined_ref[0, 0 : YLO * 96].astype(f32)
    for x in range(1, X):
        total = total + joined_ref[x, 0 : YLO * 96].astype(f32)
    half_ref[...] = total.astype(bf16)
    for x in range(X):
        for k in range(9):
            at, col = YLO * 96 + k * ROWS, x * COLS + k * 128
            average = joined_ref[X_ORDER.index(x), at : at + ROWS].astype(f32)
            moved = nesterov * momentum_ref[:, col : col + 128] + average
            new_momentum_ref[:, col : col + 128] = moved
            new_params_ref[:, col : col + 128] = params_ref[:, col : col + 128] - outer_rate * (
                average + nesterov * moved
            )


def placing(whole_ref, out_ref):
    zr = lax.axis_index("zr")
    for core in range(CORE):
        near_zr = neighbour_zr(core)
        for place in range(3):
            zr_of = zr if place == 2 else near_zr
            quarter = core if place == 2 else place
            for ylo in range(YLO):
                for low in range(2):
                    row = (low * ZR + zr_of) * 64 + (quarter * YLO + ylo) * 16
                    at = ylo * 96 + (low * 3 + place) * 16
                    out_ref[pl.ds(pl.multiple_of(row, 16), 16)] = whole_ref[core, at : at + 16]


def per_device(pseudo_grad, compensation, params, momentum, probe):
    x = lax.axis_index("x")

    grads, carried = (pltpu.with_memory_space_constraint(a, pltpu.HBM) for a in (pseudo_grad, compensation))
    copies, lent = pl.pallas_call(
        opening,
        out_shape=(jax.ShapeDtypeStruct((YLO * ZQ, 16, COLS), bf16), SUMS),
        in_specs=[ANY] * 3,
        out_specs=(ANY, VMEM),
        scratch_shapes=[
            pltpu.VMEM((YLO, 16, COLS), bf16),
            *SUMS_SCRATCH,
            pltpu.SemaphoreType.DMA((YLO + YLO * ZQ,)),
            pltpu.SemaphoreType.DMA((2, X)),
        ],
        name="opening",
        compiler_params=SMALL,
    )(pltpu.with_memory_space_constraint(probe, pltpu.HBM), grads, carried)
    far = exchange(copies, ("ylo", "zq", "zr"), FAR_ORDERS)
    lot = lax.all_gather(far, "core", axis=0)
    neighbours = [(z, z + 1) for z in range(0, Z, 2)] + [(Z + z, Z + (z + 1) % Z) for z in range(1, Z, 2)]
    near = swapped(lot, ("core", "zq", "zr"), neighbours)

    partners = swapped(lent, "core", [(0, 1)])
    kept = pl.pallas_call(
        own_rows,
        out_shape=SUMS,
        in_specs=[ANY] * 2,
        out_specs=VMEM,
        scratch_shapes=[*SUMS_SCRATCH, pltpu.SemaphoreType.DMA((2, X))],
        name="kept",
        compiler_params=SMALL,
    )(grads, carried)
    pair = (partners.astype(f32) + kept).astype(bf16)
    decayed = (params - (outer_rate * nesterov * nesterov) * momentum).astype(bf16)
    both = jnp.concatenate([pair, decayed], axis=0)

    def share(i):
        return lax.dynamic_slice_in_dim(both, lax.bitwise_xor(x, i) * COLS, COLS, axis=1)

    arrived = [share(0)]
    for i in range(1, X):
        arrived.append(swapped(share(i), "x", [(j, j ^ i) for j in range(X) if j < j ^ i]))
    average = sum(a[: X * ROWS].astype(f32) for a in arrived) / (X * CORE)
    places = jnp.stack([a[X * ROWS :] for a in arrived])
    base = jnp.concatenate([taken(places, lax.bitwise_xor(x, i)) for i in range(X)]).astype(f32)
    weights = (base - (outer_rate * (1 + nesterov)) * average).astype(bf16)

    two = lax.all_gather(weights, "ylo", axis=0)
    local_weights = lax.all_gather(two, "core", axis=0)
    chunks = pl.pallas_call(
        product,
        out_shape=jax.ShapeDtypeStruct((YHI * YLO, 96, 128), bf16),
        in_specs=[VMEM] * 3,
        out_specs=VMEM,
        scratch_shapes=[pltpu.VMEM((YLO, 128, COLS), bf16), pltpu.VMEM((3 * YLO * ZQ * 16, COLS), bf16)],
        name="product",
        compiler_params=SMALL,
    )(near, far, local_weights.reshape(CORE * YLO, X * ROWS, COLS))
    parts = exchange(chunks, ("yhi", "ylo"), [Y_ORDER])
    sent = pl.pallas_call(
        part_sums,
        out_shape=jax.ShapeDtypeStruct((X, YLO * 96 + 9 * ROWS, 128), bf16),
        in_specs=[VMEM] * 2,
        out_specs=VMEM,
        name="part_sums",
        compiler_params=SMALL,
    )(parts, average.astype(bf16))
    joined = exchange(sent, "x", [X_ORDER])
    half, new_params, new_momentum = pl.pallas_call(
        updates,
        out_shape=(
            jax.ShapeDtypeStruct((YLO * 96, 128), bf16),
            jax.ShapeDtypeStruct(params.shape, f32),
            jax.ShapeDtypeStruct(momentum.shape, f32),
        ),
        in_specs=[VMEM] * 3,
        out_specs=(VMEM,) * 3,
        name="updates",
        compiler_params=SMALL,
    )(joined, params, momentum)
    whole = lax.all_gather(half, "core", axis=0)
    probe_out = pl.pallas_call(
        placing,
        out_shape=jax.ShapeDtypeStruct((384, 128), bf16),
        in_specs=[VMEM],
        out_specs=VMEM,
        name="placing",
        compiler_params=SMALL,
    )(whole)
    return new_params, new_momentum, probe_out


def solution(mesh):
    fine = Mesh(
        mesh.devices.reshape(X, CORE, YLO, ZQ, ZR, YHI), ("x", "core", "ylo", "zq", "zr", "yhi")
    )
    whole, rows = ("x", "core"), ("ylo", "zq", "zr")
    shard = P((*rows, *whole), "yhi")
    in_specs = (P(whole, rows, "yhi"), P(whole, rows, "yhi"), shard, shard, P(rows, "yhi"))
    out_specs = (shard, shard, P("yhi", rows))

    return jax.shard_map(per_device, mesh=fine, in_specs=in_specs, out_specs=out_specs, check_vma=False)
```

```python
import jax
import jax.numpy as jnp
from jax import lax
from jax.experimental import pallas as pl
from jax.experimental.pallas import tpu as pltpu
from jax.sharding import Mesh
from jax.sharding import PartitionSpec as P


outer_rate = 0.7
nesterov = 0.9
f32, bf16 = jnp.float32, jnp.bfloat16

X, CORE, YLO, ZQ, ZR, YHI = 4, 2, 2, 4, 3, 4
Z = ZQ * ZR
Y_ORDER = [4, 3, 2, 1, 0, 7, 6, 5]
X_ORDER = [2, 0, 1, 3]
ROWS = 16
COLS = 1152


def exchange(tiles, axes, orders):
    return lax.all_to_all(tiles, axes, split_axis=0, concat_axis=0, tiled=True, axis_index_groups=orders)


LEADS = (3, 3, 2)
FAR_ORDERS = [
    [(ylo * ZQ + (lead + n) % ZQ) * ZR + zr for ylo in range(YLO) for n in range(ZQ)] for zr, lead in enumerate(LEADS)
]


def far_place(ylo, zq, zr):
    lead = jnp.where(zr == 0, LEADS[0], jnp.where(zr == 1, LEADS[1], LEADS[2]))
    return ylo * ZQ + lax.rem(zq + ZQ - lead, ZQ)


def swapped(x, axes, pairs):
    return lax.ppermute(x, axes, [*pairs, *((j, i) for i, j in pairs)])


def taken(tiles, i):
    return lax.dynamic_index_in_dim(tiles, i, 0, keepdims=False)


VMEM = pl.BlockSpec(memory_space=pltpu.VMEM)
ANY = pl.BlockSpec(memory_space=pltpu.HBM)
SMALL = pltpu.CompilerParams(vmem_limit_bytes=8 << 20)


def started(other, grads_ref, carried_ref, grad_ref, carry_ref, sems):
    core = lax.axis_index("core")
    half = 1 - core if other else core
    copies = []
    for x in range(X):
        row = pl.multiple_of((x * CORE + half) * ROWS, 16)
        pair = (
            pltpu.make_async_copy(grads_ref.at[0, pl.ds(row, ROWS)], grad_ref.at[x], sems.at[0, x]),
            pltpu.make_async_copy(carried_ref.at[0, pl.ds(row, ROWS)], carry_ref.at[x], sems.at[1, x]),
        )
        for copy in pair:
            copy.start()
        copies.append(pair)
    return copies


def added(copies, sums_ref, grad_ref, carry_ref):
    for x in range(X):
        for copy in copies[x]:
            copy.wait()
        sums_ref[x * ROWS : (x + 1) * ROWS] = (grad_ref[x].astype(f32) + carry_ref[x]).astype(bf16)


def opening(probe_ref, grads_ref, carried_ref, copies_ref, lent_ref, kept_ref, grad_ref, carry_ref, sems, sums_sems):
    core, at = lax.axis_index("core"), pl.multiple_of(lax.axis_index("x") * COLS, 128)
    loads, stores = [], []
    for ylo in range(YLO):
        row = pl.multiple_of((core * YLO + ylo) * 16, 16)
        source = probe_ref.at[pl.ds(row, 16), pl.ds(at, COLS)]
        loads.append(pltpu.make_async_copy(source, kept_ref.at[ylo], sems.at[ylo]))
        loads[-1].start()
    copies = started(True, grads_ref, carried_ref, grad_ref, carry_ref, sums_sems)
    for ylo in range(YLO):
        loads[ylo].wait()
        for zq in range(ZQ):
            to = far_place(ylo, zq, lax.axis_index("zr"))
            stores.append(
                pltpu.make_async_copy(kept_ref.at[ylo], copies_ref.at[to], sems.at[YLO + ylo * ZQ + zq])
            )
            stores[-1].start()
    added(copies, lent_ref, grad_ref, carry_ref)
    for store in stores:
        store.wait()


def own_rows(grads_ref, carried_ref, sums_ref, grad_ref, carry_ref, sems):
    added(started(False, grads_ref, carried_ref, grad_ref, carry_ref, sems), sums_ref, grad_ref, carry_ref)


SUMS = jax.ShapeDtypeStruct((X * ROWS, X * COLS), bf16)
SUMS_SCRATCH = [
    pltpu.VMEM((X, ROWS, X * COLS), bf16),
    pltpu.VMEM((X, ROWS, X * COLS), f32),
]


def neighbour_zr(core):
    zr = lax.axis_index("zr")
    odd = lax.rem(lax.axis_index("zq") * ZR + zr + core, 2)
    return lax.rem(zr + 1 + odd, ZR)


def product(near_ref, far_ref, gathered_ref, chunks_ref, weights_ref, rows_ref):
    for ylo in range(YLO):
        for x in range(X):
            for core in range(CORE):
                at = (x * CORE + core) * ROWS
                weights_ref[ylo, at : at + ROWS] = gathered_ref[core * YLO + ylo, x * ROWS : (x + 1) * ROWS]
    near_zr = neighbour_zr(lax.axis_index("core"))
    for place in range(3):
        for block in range(YLO * ZQ):
            row = (place * YLO * ZQ + block) * 16
            if place < 2:
                rows_ref[row : row + 16] = near_ref[place, far_place(block // ZQ, block % ZQ, near_zr)]
            else:
                rows_ref[row : row + 16] = far_ref[far_place(block // ZQ, block % ZQ, lax.axis_index("zr"))]
    for ylo in range(YLO):
        found = lax.dot_general(
            rows_ref[...], weights_ref[ylo], (((1,), (1,)), ((), ())), preferred_element_type=f32
        ).astype(bf16)
        for place in range(3):
            for block in range(YLO * ZQ):
                t, low = block // 2, block % 2
                at, row = (low * 3 + place) * 16, (place * YLO * ZQ + block) * 16
                chunks_ref[Y_ORDER.index(t * YLO + ylo), at : at + 16] = found[row : row + 16]


def part_sums(parts_ref, average_ref, sent_ref):
    for ylo in range(YLO):
        total = sum(parts_ref[Y_ORDER.index(t * YLO + ylo)].astype(f32) for t in range(YHI)).astype(bf16)
        for x in range(X):
            sent_ref[x, ylo * 96 : (ylo + 1) * 96] = total
    for x in range(X):
        for k in range(9):
            at = YLO * 96 + k * ROWS
            sent_ref[X_ORDER.index(x), at : at + ROWS] = average_ref[x * ROWS : (x + 1) * ROWS, k * 128 : (k + 1) * 128]


def halves(joined_ref, half_ref):
    half_ref[...] = sum(joined_ref[x, 0 : YLO * 96].astype(f32) for x in range(X)).astype(bf16)


def closing(whole_ref, joined_ref, params_ref, momentum_ref, new_params_ref, new_momentum_ref, out_ref):
    zr = lax.axis_index("zr")
    for core in range(CORE):
        near_zr = neighbour_zr(core)
        for place in range(3):
            zr_of = zr if place == 2 else near_zr
            quarter = core if place == 2 else place
            for ylo in range(YLO):
                for low in range(2):
                    row = (low * ZR + zr_of) * 64 + (quarter * YLO + ylo) * 16
                    at = ylo * 96 + (low * 3 + place) * 16
                    out_ref[pl.ds(pl.multiple_of(row, 16), 16)] = whole_ref[core, at : at + 16]
    for x in range(X):
        for k in range(9):
            at, col = YLO * 96 + k * ROWS, x * COLS + k * 128
            average = joined_ref[X_ORDER.index(x), at : at + ROWS].astype(f32)
            moved = nesterov * momentum_ref[:, col : col + 128] + average
            new_momentum_ref[:, col : col + 128] = moved
            new_params_ref[:, col : col + 128] = params_ref[:, col : col + 128] - outer_rate * (
                average + nesterov * moved
            )


def per_device(pseudo_grad, compensation, params, momentum, probe):
    x = lax.axis_index("x")

    grads, carried = (pltpu.with_memory_space_constraint(a, pltpu.HBM) for a in (pseudo_grad, compensation))
    copies, lent = pl.pallas_call(
        opening,
        out_shape=(jax.ShapeDtypeStruct((YLO * ZQ, 16, COLS), bf16), SUMS),
        in_specs=[ANY] * 3,
        out_specs=(ANY, VMEM),
        scratch_shapes=[
            pltpu.VMEM((YLO, 16, COLS), bf16),
            *SUMS_SCRATCH,
            pltpu.SemaphoreType.DMA((YLO + YLO * ZQ,)),
            pltpu.SemaphoreType.DMA((2, X)),
        ],
        name="opening",
        compiler_params=SMALL,
    )(pltpu.with_memory_space_constraint(probe, pltpu.HBM), grads, carried)
    far = exchange(copies, ("ylo", "zq", "zr"), FAR_ORDERS)
    lot = lax.all_gather(far, "core", axis=0)
    neighbours = [(z, z + 1) for z in range(0, Z, 2)] + [(Z + z, Z + (z + 1) % Z) for z in range(1, Z, 2)]
    near = swapped(lot, ("core", "zq", "zr"), neighbours)

    partners = swapped(lent, "core", [(0, 1)])
    kept = pl.pallas_call(
        own_rows,
        out_shape=SUMS,
        in_specs=[ANY] * 2,
        out_specs=VMEM,
        scratch_shapes=[*SUMS_SCRATCH, pltpu.SemaphoreType.DMA((2, X))],
        name="kept",
        compiler_params=SMALL,
    )(grads, carried)
    pair = (partners.astype(f32) + kept).astype(bf16)
    decayed = (params - (outer_rate * nesterov * nesterov) * momentum).astype(bf16)
    both = jnp.concatenate([pair, decayed], axis=0)

    def share(i):
        return lax.dynamic_slice_in_dim(both, lax.bitwise_xor(x, i) * COLS, COLS, axis=1)

    arrived = [share(0)]
    for i in range(1, X):
        arrived.append(swapped(share(i), "x", [(j, j ^ i) for j in range(X) if j < j ^ i]))
    average = sum(a[: X * ROWS].astype(f32) for a in arrived) / (X * CORE)
    places = jnp.stack([a[X * ROWS :] for a in arrived])
    base = jnp.concatenate([taken(places, lax.bitwise_xor(x, i)) for i in range(X)]).astype(f32)
    weights = (base - (outer_rate * (1 + nesterov)) * average).astype(bf16)

    two = lax.all_gather(weights, "ylo", axis=0)
    local_weights = lax.all_gather(two, "core", axis=0)
    chunks = pl.pallas_call(
        product,
        out_shape=jax.ShapeDtypeStruct((YHI * YLO, 96, 128), bf16),
        in_specs=[VMEM] * 3,
        out_specs=VMEM,
        scratch_shapes=[pltpu.VMEM((YLO, 128, COLS), bf16), pltpu.VMEM((3 * YLO * ZQ * 16, COLS), bf16)],
        name="product",
        compiler_params=SMALL,
    )(near, far, local_weights.reshape(CORE * YLO, X * ROWS, COLS))
    parts = exchange(chunks, ("yhi", "ylo"), [Y_ORDER])
    sent = pl.pallas_call(
        part_sums,
        out_shape=jax.ShapeDtypeStruct((X, YLO * 96 + 9 * ROWS, 128), bf16),
        in_specs=[VMEM] * 2,
        out_specs=VMEM,
        name="part_sums",
        compiler_params=SMALL,
    )(parts, average.astype(bf16))
    joined = exchange(sent, "x", [X_ORDER])
    half = pl.pallas_call(
        halves,
        out_shape=jax.ShapeDtypeStruct((YLO * 96, 128), bf16),
        in_specs=[VMEM],
        out_specs=VMEM,
        name="halves",
        compiler_params=SMALL,
    )(joined)
    whole = lax.all_gather(half, "core", axis=0)
    return pl.pallas_call(
        closing,
        out_shape=(
            jax.ShapeDtypeStruct(params.shape, f32),
            jax.ShapeDtypeStruct(momentum.shape, f32),
            jax.ShapeDtypeStruct((384, 128), bf16),
        ),
        in_specs=[VMEM] * 4,
        out_specs=(VMEM,) * 3,
        name="closing",
        compiler_params=SMALL,
    )(whole, joined, params, momentum)


def solution(mesh):
    fine = Mesh(
        mesh.devices.reshape(X, CORE, YLO, ZQ, ZR, YHI), ("x", "core", "ylo", "zq", "zr", "yhi")
    )
    whole, rows = ("x", "core"), ("ylo", "zq", "zr")
    shard = P((*rows, *whole), "yhi")
    in_specs = (P(whole, rows, "yhi"), P(whole, rows, "yhi"), shard, shard, P(rows, "yhi"))
    out_specs = (shard, shard, P("yhi", rows))

    return jax.shard_map(per_device, mesh=fine, in_specs=in_specs, out_specs=out_specs, check_vma=False)
```

```python
import jax
import jax.numpy as jnp
from jax import lax
from jax.experimental import pallas as pl
from jax.experimental.pallas import tpu as pltpu
from jax.sharding import Mesh
from jax.sharding import PartitionSpec as P


outer_rate = 0.7
nesterov = 0.9
f32, bf16 = jnp.float32, jnp.bfloat16

X, CORE, YLO, ZQ, ZR, YHI = 4, 2, 2, 4, 3, 4
Z = ZQ * ZR
Y_ORDER = [4, 3, 2, 1, 0, 7, 6, 5]
X_ORDER = [2, 0, 3, 1]
ROWS = 16
COLS = 1152


def exchange(tiles, axes, orders):
    return lax.all_to_all(tiles, axes, split_axis=0, concat_axis=0, tiled=True, axis_index_groups=orders)


LEADS = (3, 0, 0)
FAR_ORDERS = [
    [(ylo * ZQ + (lead + n) % ZQ) * ZR + zr for ylo in range(YLO) for n in range(ZQ)] for zr, lead in enumerate(LEADS)
]


def lead_of(zr):
    return jnp.where(zr == 0, LEADS[0], jnp.where(zr == 1, LEADS[1], LEADS[2]))


def far_place(ylo, zq, zr):
    return ylo * ZQ + lax.rem(zq + ZQ - lead_of(zr), ZQ)


def swapped(x, axes, pairs):
    return lax.ppermute(x, axes, [*pairs, *((j, i) for i, j in pairs)])


def taken(tiles, i):
    return lax.dynamic_index_in_dim(tiles, i, 0, keepdims=False)


VMEM = pl.BlockSpec(memory_space=pltpu.VMEM)
ANY = pl.BlockSpec(memory_space=pltpu.HBM)
SMALL = pltpu.CompilerParams(vmem_limit_bytes=8 << 20)


def started(other, grads_ref, carried_ref, grad_ref, carry_ref, sems):
    core = lax.axis_index("core")
    half = 1 - core if other else core
    copies = []
    for x in range(X):
        row = pl.multiple_of((x * CORE + half) * ROWS, 16)
        pair = (
            pltpu.make_async_copy(grads_ref.at[0, pl.ds(row, ROWS)], grad_ref.at[x], sems.at[0, x]),
            pltpu.make_async_copy(carried_ref.at[0, pl.ds(row, ROWS)], carry_ref.at[x], sems.at[1, x]),
        )
        for copy in pair:
            copy.start()
        copies.append(pair)
    return copies


def added(copies, sums_ref, grad_ref, carry_ref):
    for x in range(X):
        for copy in copies[x]:
            copy.wait()
        sums_ref[x * ROWS : (x + 1) * ROWS] = (grad_ref[x].astype(f32) + carry_ref[x]).astype(bf16)


def opening(probe_ref, grads_ref, carried_ref, copies_ref, lent_ref, kept_ref, grad_ref, carry_ref, sems, sums_sems):
    core, at = lax.axis_index("core"), pl.multiple_of(lax.axis_index("x") * COLS, 128)
    loads, stores = [], []
    for ylo in range(YLO):
        row = pl.multiple_of((core * YLO + ylo) * 16, 16)
        source = probe_ref.at[pl.ds(row, 16), pl.ds(at, COLS)]
        loads.append(pltpu.make_async_copy(source, kept_ref.at[ylo], sems.at[ylo]))
        loads[-1].start()
    copies = started(True, grads_ref, carried_ref, grad_ref, carry_ref, sums_sems)
    for ylo in range(YLO):
        loads[ylo].wait()
        for zq in range(ZQ):
            to = far_place(ylo, zq, lax.axis_index("zr"))
            stores.append(
                pltpu.make_async_copy(kept_ref.at[ylo], copies_ref.at[to], sems.at[YLO + ylo * ZQ + zq])
            )
            stores[-1].start()
    added(copies, lent_ref, grad_ref, carry_ref)
    for store in stores:
        store.wait()


def own_rows(grads_ref, carried_ref, sums_ref, grad_ref, carry_ref, sems):
    added(started(False, grads_ref, carried_ref, grad_ref, carry_ref, sems), sums_ref, grad_ref, carry_ref)


SUMS = jax.ShapeDtypeStruct((X * ROWS, X * COLS), bf16)
SUMS_SCRATCH = [
    pltpu.VMEM((X, ROWS, X * COLS), bf16),
    pltpu.VMEM((X, ROWS, X * COLS), f32),
]


def neighbour_zr(core):
    zr = lax.axis_index("zr")
    odd = lax.rem(lax.axis_index("zq") * ZR + zr + core, 2)
    return lax.rem(zr + 1 + odd, ZR)


def product(near_ref, far_ref, gathered_ref, chunks_ref, weights_ref):
    for ylo in range(YLO):
        for x in range(X):
            for core in range(CORE):
                at = ylo * 128 + (x * CORE + core) * ROWS
                weights_ref[at : at + ROWS] = gathered_ref[core * YLO + ylo, x * ROWS : (x + 1) * ROWS]
    near_lead = lead_of(neighbour_zr(lax.axis_index("core")))
    own_lead = lead_of(lax.axis_index("zr"))
    for place in range(3):
        ref, lead = (near_ref.at[place], near_lead) if place < 2 else (far_ref, own_lead)
        found = lax.dot_general(
            ref[...].reshape(YLO * ZQ * 16, COLS), weights_ref[...], (((1,), (1,)), ((), ())), preferred_element_type=f32
        ).astype(bf16)
        for n in range(ZQ):
            zq = lax.rem(n + lead, ZQ)
            at = pl.multiple_of((lax.rem(zq, 2) * 3 + place) * 16, 16)
            for ylo in range(YLO):
                row = (ylo * ZQ + n) * 16
                for side in range(YLO):
                    low, high = (Y_ORDER.index((ylo * 2 + half) * YLO + side) for half in range(2))
                    chunks_ref[jnp.where(zq < 2, low, high), pl.ds(at, 16)] = found[
                        row : row + 16, side * 128 : (side + 1) * 128
                    ]


def part_sums(parts_ref, average_ref, sent_ref):
    for ylo in range(YLO):
        total = sum(parts_ref[Y_ORDER.index(t * YLO + ylo)].astype(f32) for t in range(YHI)).astype(bf16)
        for x in range(X):
            sent_ref[x, ylo * 96 : (ylo + 1) * 96] = total
    for x in range(X):
        for k in range(9):
            at = YLO * 96 + k * ROWS
            sent_ref[X_ORDER.index(x), at : at + ROWS] = average_ref[x * ROWS : (x + 1) * ROWS, k * 128 : (k + 1) * 128]


def halves(joined_ref, half_ref):
    half_ref[...] = sum(joined_ref[x, 0 : YLO * 96].astype(f32) for x in range(X)).astype(bf16)


def closing(whole_ref, joined_ref, params_ref, momentum_ref, new_params_ref, new_momentum_ref, out_ref):
    zr = lax.axis_index("zr")
    for core in range(CORE):
        near_zr = neighbour_zr(core)
        for place in range(3):
            zr_of = zr if place == 2 else near_zr
            quarter = core if place == 2 else place
            for ylo in range(YLO):
                for low in range(2):
                    row = (low * ZR + zr_of) * 64 + (quarter * YLO + ylo) * 16
                    at = ylo * 96 + (low * 3 + place) * 16
                    out_ref[pl.ds(pl.multiple_of(row, 16), 16)] = whole_ref[core, at : at + 16]
    for x in range(X):
        for k in range(9):
            at, col = YLO * 96 + k * ROWS, x * COLS + k * 128
            average = joined_ref[X_ORDER.index(x), at : at + ROWS].astype(f32)
            moved = nesterov * momentum_ref[:, col : col + 128] + average
            new_momentum_ref[:, col : col + 128] = moved
            new_params_ref[:, col : col + 128] = params_ref[:, col : col + 128] - outer_rate * (
                average + nesterov * moved
            )


def per_device(pseudo_grad, compensation, params, momentum, probe):
    x = lax.axis_index("x")

    grads, carried = (pltpu.with_memory_space_constraint(a, pltpu.HBM) for a in (pseudo_grad, compensation))
    copies, lent = pl.pallas_call(
        opening,
        out_shape=(jax.ShapeDtypeStruct((YLO * ZQ, 16, COLS), bf16), SUMS),
        in_specs=[ANY] * 3,
        out_specs=(ANY, VMEM),
        scratch_shapes=[
            pltpu.VMEM((YLO, 16, COLS), bf16),
            *SUMS_SCRATCH,
            pltpu.SemaphoreType.DMA((YLO + YLO * ZQ,)),
            pltpu.SemaphoreType.DMA((2, X)),
        ],
        name="opening",
        compiler_params=SMALL,
    )(pltpu.with_memory_space_constraint(probe, pltpu.HBM), grads, carried)
    far = exchange(copies, ("ylo", "zq", "zr"), FAR_ORDERS)
    lot = lax.all_gather(far, "core", axis=0)
    neighbours = [(z, z + 1) for z in range(0, Z, 2)] + [(Z + z, Z + (z + 1) % Z) for z in range(1, Z, 2)]
    near = swapped(lot, ("core", "zq", "zr"), neighbours)

    partners = swapped(lent, "core", [(0, 1)])
    kept = pl.pallas_call(
        own_rows,
        out_shape=SUMS,
        in_specs=[ANY] * 2,
        out_specs=VMEM,
        scratch_shapes=[*SUMS_SCRATCH, pltpu.SemaphoreType.DMA((2, X))],
        name="kept",
        compiler_params=SMALL,
    )(grads, carried)
    pair = (partners.astype(f32) + kept).astype(bf16)
    decayed = (params - (outer_rate * nesterov * nesterov) * momentum).astype(bf16)
    both = jnp.concatenate([pair, decayed], axis=0)

    def share(i):
        return lax.dynamic_slice_in_dim(both, lax.bitwise_xor(x, i) * COLS, COLS, axis=1)

    arrived = [share(0)]
    for i in range(1, X):
        arrived.append(swapped(share(i), "x", [(j, j ^ i) for j in range(X) if j < j ^ i]))
    average = sum(a[: X * ROWS].astype(f32) for a in arrived) / (X * CORE)
    places = jnp.stack([a[X * ROWS :] for a in arrived])
    base = jnp.concatenate([taken(places, lax.bitwise_xor(x, i)) for i in range(X)]).astype(f32)
    weights = (base - (outer_rate * (1 + nesterov)) * average).astype(bf16)

    two = lax.all_gather(weights, "ylo", axis=0)
    local_weights = lax.all_gather(two, "core", axis=0)
    chunks = pl.pallas_call(
        product,
        out_shape=jax.ShapeDtypeStruct((YHI * YLO, 96, 128), bf16),
        in_specs=[VMEM] * 3,
        out_specs=VMEM,
        scratch_shapes=[pltpu.VMEM((YLO * 128, COLS), bf16)],
        name="product",
        compiler_params=SMALL,
    )(near, far, local_weights.reshape(CORE * YLO, X * ROWS, COLS))
    parts = exchange(chunks, ("yhi", "ylo"), [Y_ORDER])
    sent = pl.pallas_call(
        part_sums,
        out_shape=jax.ShapeDtypeStruct((X, YLO * 96 + 9 * ROWS, 128), bf16),
        in_specs=[VMEM] * 2,
        out_specs=VMEM,
        name="part_sums",
        compiler_params=SMALL,
    )(parts, average.astype(bf16))
    joined = exchange(sent, "x", [X_ORDER])
    half = pl.pallas_call(
        halves,
        out_shape=jax.ShapeDtypeStruct((YLO * 96, 128), bf16),
        in_specs=[VMEM],
        out_specs=VMEM,
        name="halves",
        compiler_params=SMALL,
    )(joined)
    whole = lax.all_gather(half, "core", axis=0)
    return pl.pallas_call(
        closing,
        out_shape=(
            jax.ShapeDtypeStruct(params.shape, f32),
            jax.ShapeDtypeStruct(momentum.shape, f32),
            jax.ShapeDtypeStruct((384, 128), bf16),
        ),
        in_specs=[VMEM] * 4,
        out_specs=(VMEM,) * 3,
        name="closing",
        compiler_params=SMALL,
    )(whole, joined, params, momentum)


def solution(mesh):
    fine = Mesh(
        mesh.devices.reshape(X, CORE, YLO, ZQ, ZR, YHI), ("x", "core", "ylo", "zq", "zr", "yhi")
    )
    whole, rows = ("x", "core"), ("ylo", "zq", "zr")
    shard = P((*rows, *whole), "yhi")
    in_specs = (P(whole, rows, "yhi"), P(whole, rows, "yhi"), shard, shard, P(rows, "yhi"))
    out_specs = (shard, shard, P("yhi", rows))

    return jax.shard_map(per_device, mesh=fine, in_specs=in_specs, out_specs=out_specs, check_vma=False)
```

```python
import jax
import jax.numpy as jnp
from jax import lax
from jax.experimental import pallas as pl
from jax.experimental.pallas import tpu as pltpu
from jax.sharding import Mesh
from jax.sharding import PartitionSpec as P


outer_rate = 0.7
nesterov = 0.9
f32, bf16 = jnp.float32, jnp.bfloat16

X, CORE, YLO, ZQ, ZR, YHI = 4, 2, 2, 4, 3, 4
Z = ZQ * ZR
Y_ORDER = [4, 3, 2, 1, 0, 7, 6, 5]
X_ORDER = [2, 0, 3, 1]
ROWS = 16
COLS = 1152


def exchange(tiles, axes, orders):
    return lax.all_to_all(tiles, axes, split_axis=0, concat_axis=0, tiled=True, axis_index_groups=orders)


LEADS = (3, 0, 0)
FAR_ORDERS = [
    [(ylo * ZQ + (lead + n) % ZQ) * ZR + zr for ylo in range(YLO) for n in range(ZQ)] for zr, lead in enumerate(LEADS)
]


def lead_of(zr):
    return jnp.where(zr == 0, LEADS[0], jnp.where(zr == 1, LEADS[1], LEADS[2]))


def far_place(ylo, zq, zr):
    return ylo * ZQ + lax.rem(zq + ZQ - lead_of(zr), ZQ)


def swapped(x, axes, pairs):
    return lax.ppermute(x, axes, [*pairs, *((j, i) for i, j in pairs)])


def taken(tiles, i):
    return lax.dynamic_index_in_dim(tiles, i, 0, keepdims=False)


VMEM = pl.BlockSpec(memory_space=pltpu.VMEM)
ANY = pl.BlockSpec(memory_space=pltpu.HBM)
SMALL = pltpu.CompilerParams(vmem_limit_bytes=8 << 20)


def started(other, grads_ref, carried_ref, grad_ref, carry_ref, sems):
    core = lax.axis_index("core")
    half = 1 - core if other else core
    copies = []
    for x in range(X):
        row = pl.multiple_of((x * CORE + half) * ROWS, 16)
        pair = (
            pltpu.make_async_copy(grads_ref.at[0, pl.ds(row, ROWS)], grad_ref.at[x], sems.at[0, x]),
            pltpu.make_async_copy(carried_ref.at[0, pl.ds(row, ROWS)], carry_ref.at[x], sems.at[1, x]),
        )
        copies.append(pair)
    for n in (1, 0):
        for pair in copies:
            pair[n].start()
    return copies


def added(copies, sums_ref, grad_ref, carry_ref):
    for x in range(X):
        for copy in copies[x]:
            copy.wait()
        sums_ref[x * ROWS : (x + 1) * ROWS] = (grad_ref[x].astype(f32) + carry_ref[x]).astype(bf16)


def opening(probe_ref, grads_ref, carried_ref, copies_ref, lent_ref, kept_ref, grad_ref, carry_ref, sems, sums_sems):
    core, at = lax.axis_index("core"), pl.multiple_of(lax.axis_index("x") * COLS, 128)
    loads, stores = [], []
    for ylo in range(YLO):
        row = pl.multiple_of((core * YLO + ylo) * 16, 16)
        source = probe_ref.at[pl.ds(row, 16), pl.ds(at, COLS)]
        loads.append(pltpu.make_async_copy(source, kept_ref.at[ylo], sems.at[ylo]))
        loads[-1].start()
    copies = started(True, grads_ref, carried_ref, grad_ref, carry_ref, sums_sems)
    for ylo in range(YLO):
        loads[ylo].wait()
        for zq in range(ZQ):
            to = far_place(ylo, zq, lax.axis_index("zr"))
            stores.append(
                pltpu.make_async_copy(kept_ref.at[ylo], copies_ref.at[to], sems.at[YLO + ylo * ZQ + zq])
            )
            stores[-1].start()
    added(copies, lent_ref, grad_ref, carry_ref)
    for store in stores:
        store.wait()


def own_rows(grads_ref, carried_ref, sums_ref, grad_ref, carry_ref, sems):
    added(started(False, grads_ref, carried_ref, grad_ref, carry_ref, sems), sums_ref, grad_ref, carry_ref)


SUMS = jax.ShapeDtypeStruct((X * ROWS, X * COLS), bf16)
SUMS_SCRATCH = [
    pltpu.VMEM((X, ROWS, X * COLS), bf16),
    pltpu.VMEM((X, ROWS, X * COLS), f32),
]


def neighbour_zr(core):
    zr = lax.axis_index("zr")
    odd = lax.rem(lax.axis_index("zq") * ZR + zr + core, 2)
    return lax.rem(zr + 1 + odd, ZR)


def product(near_ref, far_ref, gathered_ref, chunks_ref, weights_ref):
    for ylo in range(YLO):
        for x in range(X):
            for core in range(CORE):
                at = ylo * 128 + (x * CORE + core) * ROWS
                weights_ref[at : at + ROWS] = gathered_ref[core * YLO + ylo, x * ROWS : (x + 1) * ROWS]
    near_lead = lead_of(neighbour_zr(lax.axis_index("core")))
    own_lead = lead_of(lax.axis_index("zr"))
    for place in range(3):
        ref, lead = (near_ref.at[place], near_lead) if place < 2 else (far_ref, own_lead)
        found = lax.dot_general(
            ref[...].reshape(YLO * ZQ * 16, COLS), weights_ref[...], (((1,), (1,)), ((), ())), preferred_element_type=f32
        ).astype(bf16)
        for n in range(ZQ):
            zq = lax.rem(n + lead, ZQ)
            at = pl.multiple_of((lax.rem(zq, 2) * 3 + place) * 16, 16)
            for ylo in range(YLO):
                row = (ylo * ZQ + n) * 16
                for side in range(YLO):
                    low, high = (Y_ORDER.index((ylo * 2 + half) * YLO + side) for half in range(2))
                    chunks_ref[jnp.where(zq < 2, low, high), pl.ds(at, 16)] = found[
                        row : row + 16, side * 128 : (side + 1) * 128
                    ]


def part_sums(parts_ref, average_ref, sent_ref):
    for ylo in range(YLO):
        total = sum(parts_ref[Y_ORDER.index(t * YLO + ylo)].astype(f32) for t in range(YHI)).astype(bf16)
        for x in range(X):
            sent_ref[x, ylo * 96 : (ylo + 1) * 96] = total
    for x in range(X):
        for k in range(9):
            at = YLO * 96 + k * ROWS
            sent_ref[X_ORDER.index(x), at : at + ROWS] = average_ref[x * ROWS : (x + 1) * ROWS, k * 128 : (k + 1) * 128]


def halves(joined_ref, half_ref):
    half_ref[...] = sum(joined_ref[x, 0 : YLO * 96].astype(f32) for x in range(X)).astype(bf16)


def closing(whole_ref, joined_ref, params_ref, momentum_ref, new_params_ref, new_momentum_ref, out_ref):
    zr = lax.axis_index("zr")
    for core in range(CORE):
        near_zr = neighbour_zr(core)
        for place in range(3):
            zr_of = zr if place == 2 else near_zr
            quarter = core if place == 2 else place
            for ylo in range(YLO):
                for low in range(2):
                    row = (low * ZR + zr_of) * 64 + (quarter * YLO + ylo) * 16
                    at = ylo * 96 + (low * 3 + place) * 16
                    out_ref[pl.ds(pl.multiple_of(row, 16), 16)] = whole_ref[core, at : at + 16]
    for x in range(X):
        for k in range(9):
            at, col = YLO * 96 + k * ROWS, x * COLS + k * 128
            average = joined_ref[X_ORDER.index(x), at : at + ROWS].astype(f32)
            moved = nesterov * momentum_ref[:, col : col + 128] + average
            new_momentum_ref[:, col : col + 128] = moved
            new_params_ref[:, col : col + 128] = params_ref[:, col : col + 128] - outer_rate * (
                average + nesterov * moved
            )


def per_device(pseudo_grad, compensation, params, momentum, probe):
    x = lax.axis_index("x")

    grads, carried = (pltpu.with_memory_space_constraint(a, pltpu.HBM) for a in (pseudo_grad, compensation))
    copies, lent = pl.pallas_call(
        opening,
        out_shape=(jax.ShapeDtypeStruct((YLO * ZQ, 16, COLS), bf16), SUMS),
        in_specs=[ANY] * 3,
        out_specs=(ANY, VMEM),
        scratch_shapes=[
            pltpu.VMEM((YLO, 16, COLS), bf16),
            *SUMS_SCRATCH,
            pltpu.SemaphoreType.DMA((YLO + YLO * ZQ,)),
            pltpu.SemaphoreType.DMA((2, X)),
        ],
        name="opening",
        compiler_params=SMALL,
    )(pltpu.with_memory_space_constraint(probe, pltpu.HBM), grads, carried)
    far = exchange(copies, ("ylo", "zq", "zr"), FAR_ORDERS)
    lot = lax.all_gather(far, "core", axis=0)
    neighbours = [(z, z + 1) for z in range(0, Z, 2)] + [(Z + z, Z + (z + 1) % Z) for z in range(1, Z, 2)]
    near = swapped(lot, ("core", "zq", "zr"), neighbours)

    partners = swapped(lent, "core", [(0, 1)])
    kept = pl.pallas_call(
        own_rows,
        out_shape=SUMS,
        in_specs=[ANY] * 2,
        out_specs=VMEM,
        scratch_shapes=[*SUMS_SCRATCH, pltpu.SemaphoreType.DMA((2, X))],
        name="kept",
        compiler_params=SMALL,
    )(grads, carried)
    pair = (partners.astype(f32) + kept).astype(bf16)
    decayed = (params - (outer_rate * nesterov * nesterov) * momentum).astype(bf16)
    both = jnp.concatenate([pair, decayed], axis=0)

    def share(i):
        return lax.dynamic_slice_in_dim(both, lax.bitwise_xor(x, i) * COLS, COLS, axis=1)

    arrived = [share(0)]
    for i in range(1, X):
        arrived.append(swapped(share(i), "x", [(j, j ^ i) for j in range(X) if j < j ^ i]))
    average = sum(a[: X * ROWS].astype(f32) for a in arrived) / (X * CORE)
    places = jnp.stack([a[X * ROWS :] for a in arrived])
    base = jnp.concatenate([taken(places, lax.bitwise_xor(x, i)) for i in range(X)]).astype(f32)
    weights = (base - (outer_rate * (1 + nesterov)) * average).astype(bf16)

    two = lax.all_gather(weights, "ylo", axis=0)
    local_weights = lax.all_gather(two, "core", axis=0)
    chunks = pl.pallas_call(
        product,
        out_shape=jax.ShapeDtypeStruct((YHI * YLO, 96, 128), bf16),
        in_specs=[VMEM] * 3,
        out_specs=VMEM,
        scratch_shapes=[pltpu.VMEM((YLO * 128, COLS), bf16)],
        name="product",
        compiler_params=SMALL,
    )(near, far, local_weights.reshape(CORE * YLO, X * ROWS, COLS))
    parts = exchange(chunks, ("yhi", "ylo"), [Y_ORDER])
    sent = pl.pallas_call(
        part_sums,
        out_shape=jax.ShapeDtypeStruct((X, YLO * 96 + 9 * ROWS, 128), bf16),
        in_specs=[VMEM] * 2,
        out_specs=VMEM,
        name="part_sums",
        compiler_params=SMALL,
    )(parts, average.astype(bf16))
    joined = exchange(sent, "x", [X_ORDER])
    half = pl.pallas_call(
        halves,
        out_shape=jax.ShapeDtypeStruct((YLO * 96, 128), bf16),
        in_specs=[VMEM],
        out_specs=VMEM,
        name="halves",
        compiler_params=SMALL,
    )(joined)
    whole = lax.all_gather(half, "core", axis=0)
    return pl.pallas_call(
        closing,
        out_shape=(
            jax.ShapeDtypeStruct(params.shape, f32),
            jax.ShapeDtypeStruct(momentum.shape, f32),
            jax.ShapeDtypeStruct((384, 128), bf16),
        ),
        in_specs=[VMEM] * 4,
        out_specs=(VMEM,) * 3,
        name="closing",
        compiler_params=SMALL,
    )(whole, joined, params, momentum)


def solution(mesh):
    fine = Mesh(
        mesh.devices.reshape(X, CORE, YLO, ZQ, ZR, YHI), ("x", "core", "ylo", "zq", "zr", "yhi")
    )
    whole, rows = ("x", "core"), ("ylo", "zq", "zr")
    shard = P((*rows, *whole), "yhi")
    in_specs = (P(whole, rows, "yhi"), P(whole, rows, "yhi"), shard, shard, P(rows, "yhi"))
    out_specs = (shard, shard, P("yhi", rows))

    return jax.shard_map(per_device, mesh=fine, in_specs=in_specs, out_specs=out_specs, check_vma=False)
```
